32 devices in a mesh: gx: 4 (over z), gy: 4 (over y, x), gz: 2 (over core).
Axes of the slice: x: 2, y: 2, z: 4, core: 2. Of those that a mesh axis runs over, the one named last changes fastest.
Arguments:
- volume: float32 [32, 256, 4096], P('gz', 'gy', 'gx'), may hold values from -24 to 24
Outputs:
- level_one: float32 [16, 128, 2048], P('gz', 'gy', 'gx')
- level_two: float32 [8, 64, 1024], P('gz', 'gy', 'gx')
- level_three: float32 [4, 32, 512], P('gz', 'gy', 'gx')
The draws below stay inside these ranges and needn't reach their ends.
All inputs are finite; a program needn't handle non-finite values.
Results may differ from the reference program's by a relative error of at most 0.00002.
Values sent between devices are 32-bit elements; how exact they have to be, the bound alone decides.
A program may use at most 64 MiB of HBM per device.

```python
import jax
import jax.numpy as jnp
from jax import lax

NX = 4096
NY = 256
NZ = 32


def shard_levels(stream_key, shape, split, smallest, largest):
    level = 1.0
    for dim, shards_of in split:
        draws = jax.random.uniform(jax.random.fold_in(jax.random.fold_in(stream_key, 6), dim), (shards_of,), jnp.float32, smallest / len(split), largest / len(split))
        level = level * jnp.repeat(jnp.exp(draws), shape[dim] // shards_of).reshape((-1,) + (1,) * (len(shape) - 1 - dim))
    return level


def gaussian(rng, dims, deviation, most, cuts=(), kind=jnp.bfloat16):
    result = deviation * jax.random.normal(rng, dims, jnp.float32)
    if cuts:
        result = result * shard_levels(rng, dims, cuts, -0.22, 0.18)
    return jnp.clip(result, -most, most).astype(kind)


def setup_inputs(seed: int = 0) -> dict:
    streams_of = jax.random.split(jax.random.key(seed), 2)
    return {
        "volume": gaussian(streams_of[0], (NZ, NY, NX), 4.0, 24.0, ((0, 2), (1, 4), (2, 4)), jnp.float32),
    }


taps = (0.0625, 0.25, 0.375, 0.25, 0.0625)


def reduce_padded(padded, dim, count):
    total = None
    for k in range(5):
        piece = lax.slice_in_dim(padded, k, k + 2 * count - 1, 2, dim)
        term = taps[k] * piece
        total = term if total is None else total + term
    return total


def reduce_axis(field, dim):
    widths = [(0, 0), (0, 0), (0, 0)]
    widths[dim] = (2, 2)
    padded = jnp.pad(field, widths)
    return reduce_padded(padded, dim, field.shape[dim] // 2)


def level_down(field):
    return reduce_axis(reduce_axis(reduce_axis(field, 0), 1), 2)


def reference(volume):
    level_one = level_down(volume)
    level_two = level_down(level_one)
    level_three = level_down(level_two)
    return level_one, level_two, level_three
```

```python
import functools

import jax
import jax.numpy as jnp
from jax import lax
from jax.experimental import pallas as pl
from jax.experimental.pallas import tpu as pltpu
from jax.sharding import PartitionSpec as P

LANES = 128
MESH = pl.DeviceIdType.MESH
AXES = ("gz", "gy", "gx")
W0, W1, W2 = 0.0625, 0.25, 0.375


def taps_of(delta):
    far = jnp.abs(delta)
    return jnp.where(
        far == 0, W2, jnp.where(far == 1, W1, jnp.where(far == 2, W0, 0.0))
    ).astype(jnp.bfloat16)


def column_weights():
    row = lax.broadcasted_iota(jnp.int32, (LANES, LANES), 0)
    col = lax.broadcasted_iota(jnp.int32, (LANES, LANES), 1)
    before = taps_of(row - LANES - 2 * col)
    first = taps_of(row - 2 * col)
    second = taps_of(row + LANES - 2 * col)
    after = taps_of(row + 2 * LANES - 2 * col)
    half = LANES // 2
    signed_in = jnp.where(row < half, row, row - LANES)
    signed_out = jnp.where(col < half, col, col - LANES)
    same_side = (row < half) == (col < half)
    halo = taps_of(jnp.where(same_side, signed_in - 2 * signed_out, LANES))
    return before, first, second, after, halo


def split3(x):
    hi = x.astype(jnp.bfloat16)
    rest = x - hi.astype(jnp.float32)
    mid = rest.astype(jnp.bfloat16)
    lo = (rest - mid.astype(jnp.float32)).astype(jnp.bfloat16)
    return hi, mid, lo


def dots(tiles, weights):
    parts = [split3(t) for t in tiles]
    total = None
    for p in (2, 1, 0):
        lhs = jnp.concatenate([q[p] for q in parts], axis=1)
        d = jnp.dot(lhs, weights, preferred_element_type=jnp.float32)
        total = d if total is None else total + d
    return total


def kernel(sizes, nz, ny, nt, vol, out1, out2, out3,
           v, z1, z2, z3, l1, l2,
           ys_lo, ys_hi, yr_lo, yr_hi,
           t1, t2, t3, xs_lo, xs_hi, xr, wm, wh,
           load_sem, zsend, zrecv, ysend, yrecv, xsend, xrecv):
    idx = {a: lax.axis_index(a) for a in AXES}
    has_lo = {a: idx[a] > 0 for a in AXES}
    has_hi = {a: idx[a] < sizes[a] - 1 for a in AXES}
    below = {a: {a: jnp.maximum(idx[a] - 1, 0)} for a in AXES}
    above = {a: {a: jnp.minimum(idx[a] + 1, sizes[a] - 1)} for a in AXES}

    xr[...] = jnp.zeros(xr.shape, jnp.float32)
    barrier = pltpu.get_barrier_semaphore()
    for a in AXES:
        @pl.when(has_lo[a])
        def _():
            pl.semaphore_signal(barrier, inc=1, device_id=below[a], device_id_type=MESH)

        @pl.when(has_hi[a])
        def _():
            pl.semaphore_signal(barrier, inc=1, device_id=above[a], device_id_type=MESH)

    groups = ((0, 8), (ny - 8, 8), (8, ny - 16))
    loads = []
    for g, (r0, rn) in enumerate(groups):
        c = pltpu.make_async_copy(
            vol.at[:, pl.ds(r0, rn), :], v.at[pl.ds(2, nz), pl.ds(r0, rn), :], load_sem.at[g])
        c.start()
        loads.append(c)

    for z, lev in ((v, 0), (l1, 1), (l2, 2)):
        @pl.when(jnp.logical_not(has_lo["gz"]))
        def _():
            z[0:2] = jnp.zeros((2,) + z.shape[1:], jnp.float32)

        @pl.when(jnp.logical_not(has_hi["gz"]))
        def _():
            n = z.shape[0]
            z[n - 1:n] = jnp.zeros((1,) + z.shape[1:], jnp.float32)
    for lev in range(3):
        @pl.when(jnp.logical_not(has_lo["gy"]))
        def _():
            yr_lo[lev][...] = jnp.zeros(yr_lo[lev].shape, jnp.float32)

        @pl.when(jnp.logical_not(has_hi["gy"]))
        def _():
            yr_hi[lev][...] = jnp.zeros(yr_hi[lev].shape, jnp.float32)
    before, first, second, after, halo = column_weights()
    for i, m in enumerate((before, first, second, after)):
        wm[i * LANES:(i + 1) * LANES] = m
    for i, m in enumerate((before, halo, after)):
        wh[i * LANES:(i + 1) * LANES] = m

    peers = sum(has_lo[a].astype(jnp.int32) + has_hi[a].astype(jnp.int32) for a in AXES)
    pl.semaphore_wait(barrier, peers)

    pending = []

    def exchange(axis, src_lo, dst_hi, src_hi, dst_lo, send, recv, base):
        down = pltpu.make_async_remote_copy(
            src_ref=src_lo, dst_ref=dst_hi, send_sem=send.at[base], recv_sem=recv.at[base],
            device_id=below[axis], device_id_type=MESH)
        up = pltpu.make_async_remote_copy(
            src_ref=src_hi, dst_ref=dst_lo, send_sem=send.at[base + 1],
            recv_sem=recv.at[base + 1], device_id=above[axis], device_id_type=MESH)

        @pl.when(has_hi[axis])
        def _():
            up.start()

        @pl.when(has_lo[axis])
        def _():
            down.start()

        pending.append((axis, down, up))

        def wait():
            @pl.when(has_lo[axis])
            def _():
                up.wait_recv()

            @pl.when(has_hi[axis])
            def _():
                down.wait_recv()

        return wait

    wait_z = exchange(
        "gz", vol.at[pl.ds(0, 1)], v.at[pl.ds(nz + 2, 1)],
        vol.at[pl.ds(nz - 2, 2)], v.at[pl.ds(0, 2)], zsend, zrecv, 0)

    def section_sum(load, s):
        return W0 * (load(2 * s) + load(2 * s + 4)) + W1 * (load(2 * s + 1) + load(2 * s + 3)) \
            + W2 * load(2 * s + 2)

    def sections_first(s, r0, rn):
        for r in range(r0, r0 + rn, 8):
            for lt in range(nt):
                cols = slice(lt * LANES, (lt + 1) * LANES)
                z1[s, lt, 8 + r:16 + r, :] = section_sum(lambda i: v[i, r:r + 8, cols], s)

    def sections_next(src, dst, s, tiles, rows):
        for lt in range(tiles):
            dst[s, lt, 8:8 + rows, :] = section_sum(lambda i: src[i, lt], s)

    def send_rows(lev, z, rows):
        ys_hi[lev][...] = z[:, :, 6 + rows:8 + rows, :]
        ys_lo[lev][...] = z[:, :, 8:9, :]
        return exchange("gy", ys_lo[lev], yr_hi[lev], ys_hi[lev], yr_lo[lev],
                        ysend, yrecv, 2 * lev)

    def take_rows(lev, z, rows):
        z[:, :, 6:8, :] = yr_lo[lev][...]
        z[:, :, 8 + rows:9 + rows, :] = yr_hi[lev][...]

    def row_sum(z, t, s, lt, rows):
        def load(k):
            return z[s, lt, pl.ds(6 + k, rows // 2, 2), :]
        t[lt, s] = W0 * (load(0) + load(4)) + W1 * (load(1) + load(3)) + W2 * load(2)

    def tile_of(t, i):
        x = t[i]
        return x.reshape(x.shape[0] * x.shape[1], LANES)

    def main_tile(t, j, tiles):
        ids = ((2 * j - 1) % (tiles + 1), 2 * j, 2 * j + 1, 2 * j + 2)
        return dots([tile_of(t, i) for i in ids], wm[...])

    def halo_tile(t, tiles):
        out = dots([tile_of(t, i) for i in (tiles - 1, tiles, 0)], wh[...])
        lane = lax.broadcasted_iota(jnp.int32, out.shape, 1)
        keep_hi = jnp.where(has_hi["gx"], 1, 0)
        keep_lo = jnp.where(has_lo["gx"], 1, 0)
        keep = jnp.where(lane < LANES // 2, keep_hi, keep_lo)
        return jnp.where(keep > 0, out, 0.0)

    def put(l, j, x):
        n = l.shape[0] - 3
        l[2:2 + n, j] = x.reshape(n, l.shape[2], LANES)

    nz1, ny1 = nz // 2, ny // 2
    loads[0].wait()
    loads[1].wait()

    def edges(s):
        sections_first(s, 0, 8)
        sections_first(s, ny - 8, 8)

    @pl.loop(1, nz1 - 1)
    def _(s):
        edges(s)
    wait_z()
    edges(0)
    edges(nz1 - 1)
    wait_y = send_rows(0, z1, ny)
    loads[2].wait()

    @pl.loop(0, nz1)
    def _(s):
        sections_first(s, 8, ny - 16)
    wait_y()
    take_rows(0, z1, ny)

    @pl.loop(0, nz1)
    def _(s):
        row_sum(z1, t1, s, 0, ny)
        row_sum(z1, t1, s, nt - 1, ny)
    xs_lo[...] = tile_of(t1, 0).T[0:8, :]
    xs_hi[...] = tile_of(t1, nt - 1).T[LANES - 16:LANES, :]
    wait_x = exchange("gx", xs_lo, xr.at[pl.ds(0, 8)], xs_hi, xr.at[pl.ds(LANES - 16, 16)],
                      xsend, xrecv, 0)

    @pl.loop(0, nz1)
    def _(s):
        for lt in range(1, nt - 1):
            row_sum(z1, t1, s, lt, ny)
    nt1 = nt // 2
    for j in range(1, nt1 - 1):
        put(l1, j, main_tile(t1, j, nt))
    wait_x()
    t1[nt] = xr[...].T.reshape(nz1, ny1, LANES)
    put(l1, 0, main_tile(t1, 0, nt))
    put(l1, nt1 - 1, main_tile(t1, nt1 - 1, nt))
    put(l1, nt1, halo_tile(t1, nt))

    def store(l, out, tiles):
        n = out.shape[0]
        for j in range(tiles):
            out[:, :, j * LANES:(j + 1) * LANES] = l[2:2 + n, j]

    def next_level(lev, src, z, t, rows, tiles):
        n = src.shape[0] - 3
        wait = exchange("gz", src.at[pl.ds(2, 1)], src.at[pl.ds(n + 2, 1)],
                        src.at[pl.ds(n, 2)], src.at[pl.ds(0, 2)], zsend, zrecv, 2 * lev)
        for s in range(1, n // 2 - 1):
            sections_next(src, z, s, tiles + 1, rows)
        wait()
        sections_next(src, z, 0, tiles + 1, rows)
        sections_next(src, z, n // 2 - 1, tiles + 1, rows)
        wait_rows = send_rows(lev, z, rows)
        return wait_rows

    def finish_rows(lev, wait_rows, z, t, rows, tiles):
        wait_rows()
        take_rows(lev, z, rows)
        for s in range(z.shape[0]):
            for lt in range(tiles + 1):
                row_sum(z, t, s, lt, rows)

    w = next_level(1, l1, z2, t2, ny1, nt1)
    store(l1, out1, nt1)
    finish_rows(1, w, z2, t2, ny1, nt1)
    nt2, ny2 = nt1 // 2, ny1 // 2
    for j in range(nt2):
        put(l2, j, main_tile(t2, j, nt1))
    put(l2, nt2, halo_tile(t2, nt1))

    w = next_level(2, l2, z3, t3, ny2, nt2)
    store(l2, out2, nt2)
    finish_rows(2, w, z3, t3, ny2, nt2)
    nt3 = nt2 // 2
    for j in range(nt3):
        x = main_tile(t3, j, nt2)
        out3[:, :, j * LANES:(j + 1) * LANES] = x.reshape(out3.shape[0], out3.shape[1], LANES)

    for axis, down, up in pending:
        @pl.when(has_lo[axis])
        def _():
            down.wait_send()

        @pl.when(has_hi[axis])
        def _():
            up.wait_send()


def on_device(sizes, volume):
    f32 = jnp.float32
    nz, ny, nx = volume.shape
    nt = nx // LANES
    V = pltpu.VMEM
    z = [V((nz >> (l + 1), (nt >> l) + (l > 0), (ny >> l) + 16, LANES), f32) for l in range(3)]
    lv = [V((3 + (nz >> l), (nt >> l) + 1, ny >> l, LANES), f32) for l in (1, 2)]
    halo = lambda k: [V((nz >> (l + 1), (nt >> l) + (l > 0), k, LANES), f32) for l in range(3)]
    t = [V(((nt >> l) + 1, nz >> (l + 1), ny >> (l + 1), LANES), f32) for l in range(3)]
    packed = (nz >> 1) * (ny >> 1)
    dma = pltpu.SemaphoreType.DMA
    hbm = pl.BlockSpec(memory_space=pltpu.HBM)
    vmem = pl.BlockSpec(memory_space=pltpu.VMEM)
    return pl.pallas_call(
        functools.partial(kernel, sizes, nz, ny, nt),
        out_shape=tuple(
            jax.ShapeDtypeStruct((nz >> l, ny >> l, nx >> l), f32) for l in (1, 2, 3)),
        in_specs=[hbm],
        out_specs=(vmem, vmem, vmem),
        scratch_shapes=[
            V((nz + 3, ny, nx), f32), *z, *lv,
            halo(1), halo(2), halo(2), halo(1),
            *t, V((8, packed), f32), V((16, packed), f32), V((LANES, packed), f32),
            V((4 * LANES, LANES), jnp.bfloat16), V((3 * LANES, LANES), jnp.bfloat16),
            dma((3,)),
            dma((6,)), dma((6,)), dma((6,)), dma((6,)), dma((2,)), dma((2,)),
        ],
        compiler_params=pltpu.CompilerParams(
            collective_id=0, has_side_effects=True, vmem_limit_bytes=61 << 20),
        name="pyramid",
    )(volume)


def solution(mesh):
    sizes = {a: mesh.shape[a] for a in AXES}
    spec = P(*AXES)
    return jax.shard_map(
        functools.partial(on_device, sizes), mesh=mesh, in_specs=(spec,),
        out_specs=(spec, spec, spec), check_vma=False)
```

```python
import functools

import jax
import jax.numpy as jnp
from jax import lax
from jax.experimental import pallas as pl
from jax.experimental.pallas import tpu as pltpu
from jax.sharding import PartitionSpec as P

LANES = 128
MESH = pl.DeviceIdType.MESH
AXES = ("gz", "gy", "gx")
W0, W1, W2 = 0.0625, 0.25, 0.375


def taps_of(delta):
    far = jnp.abs(delta)
    return jnp.where(
        far == 0, W2, jnp.where(far == 1, W1, jnp.where(far == 2, W0, 0.0))
    ).astype(jnp.bfloat16)


def column_weights():
    row = lax.broadcasted_iota(jnp.int32, (LANES, LANES), 0)
    col = lax.broadcasted_iota(jnp.int32, (LANES, LANES), 1)
    before = taps_of(row - LANES - 2 * col)
    first = taps_of(row - 2 * col)
    second = taps_of(row + LANES - 2 * col)
    after = taps_of(row + 2 * LANES - 2 * col)
    half = LANES // 2
    signed_in = jnp.where(row < half, row, row - LANES)
    signed_out = jnp.where(col < half, col, col - LANES)
    same_side = (row < half) == (col < half)
    halo = taps_of(jnp.where(same_side, signed_in - 2 * signed_out, LANES))
    return before, first, second, after, halo


def split3(x):
    hi = x.astype(jnp.bfloat16)
    rest = x - hi.astype(jnp.float32)
    mid = rest.astype(jnp.bfloat16)
    lo = (rest - mid.astype(jnp.float32)).astype(jnp.bfloat16)
    return hi, mid, lo


def dots(tiles, weights):
    parts = [split3(t) for t in tiles]
    total = None
    for p in (2, 1, 0):
        lhs = jnp.concatenate([q[p] for q in parts], axis=1)
        d = jnp.dot(lhs, weights, preferred_element_type=jnp.float32)
        total = d if total is None else total + d
    return total


def kernel(sizes, nz, ny, nt, vol, out1, out2, out3,
           v, z, zr, ys, yr, t, l1, l2, xs_lo, xs_hi, xr, wm, wh,
           load_sem, zsend, zrecv, ysend, yrecv, xsend, xrecv):
    idx = {a: lax.axis_index(a) for a in AXES}
    has = {}
    near = {}
    for a in AXES:
        has[a, -1], has[a, 1] = idx[a] > 0, idx[a] < sizes[a] - 1
        near[a, -1] = jnp.maximum(idx[a] - 1, 0)
        near[a, 1] = jnp.minimum(idx[a] + 1, sizes[a] - 1)

    def exists(steps):
        found = None
        for a, d in steps.items():
            found = has[a, d] if found is None else jnp.logical_and(found, has[a, d])
        return found

    def device(steps):
        return {a: near[a, d] for a, d in steps.items()}

    groups = ((0, 8), (ny - 8, 8), (8, ny - 16))
    loads = []
    for g, (r0, rn) in enumerate(groups):
        c = pltpu.make_async_copy(
            vol.at[:, pl.ds(r0, rn), :], v.at[:, pl.ds(r0, rn), :], load_sem.at[g])
        c.start()
        loads.append(c)

    xr[...] = jnp.zeros(xr.shape, jnp.float32)
    for lev in range(3):
        yr[lev][...] = jnp.zeros(yr[lev].shape, jnp.float32)

    corners = [{"gz": i, "gy": j} for i in (-1, 1) for j in (-1, 1)]
    peers = [{a: d} for a in AXES for d in (-1, 1)] + corners
    barrier = pltpu.get_barrier_semaphore()
    for p in peers:
        @pl.when(exists(p))
        def _():
            pl.semaphore_signal(barrier, inc=1, device_id=device(p), device_id_type=MESH)

    for lev in range(3):
        rows = z[lev].shape[2] - 16
        edge = jnp.zeros(z[lev].shape[:2] + (8, LANES), jnp.float32)
        z[lev][:, :, 0:8, :] = edge
        z[lev][:, :, 8 + rows:16 + rows, :] = edge
    before, first, second, after, halo = column_weights()
    for i, m in enumerate((before, first, second, after)):
        wm[i * LANES:(i + 1) * LANES] = m
    for i, m in enumerate((before, halo, after)):
        wh[i * LANES:(i + 1) * LANES] = m

    pl.semaphore_wait(barrier, sum(exists(p).astype(jnp.int32) for p in peers))

    sent = []

    def send(steps, src, dst, send_sem, recv_sem):
        copy = pltpu.make_async_remote_copy(
            src_ref=src, dst_ref=dst, send_sem=send_sem, recv_sem=recv_sem,
            device_id=device(steps), device_id_type=MESH)

        @pl.when(exists(steps))
        def _():
            copy.start()
        sent.append((steps, copy))

        def wait():
            @pl.when(exists({a: -d for a, d in steps.items()}))
            def _():
                copy.wait_recv()
        return wait

    def own_sum(load, out, n):
        if isinstance(out, int) and out == n // 2:
            return W0 * load(n - 2) + W1 * load(n - 1)
        if isinstance(out, int) and out == n // 2 + 1:
            return W0 * load(0)
        c = 2 * out
        if isinstance(out, int) and out == 0:
            return W2 * load(c) + W1 * load(c + 1) + W0 * load(c + 2)
        if isinstance(out, int) and out == n // 2 - 1:
            return W0 * load(c - 2) + W1 * (load(c - 1) + load(c + 1)) + W2 * load(c)
        return W0 * (load(c - 2) + load(c + 2)) + W1 * (load(c - 1) + load(c + 1)) + W2 * load(c)

    def sections_first(out, r0, rn):
        for r in range(r0, r0 + rn, 8):
            for lt in range(nt):
                cols = slice(lt * LANES, (lt + 1) * LANES)
                z[0][out, lt, 8 + r:16 + r, :] = own_sum(lambda i: v[i, r:r + 8, cols], out, nz)

    def sections_next(lev, src, out):
        rows = src.shape[2]
        for lt in range(src.shape[1]):
            z[lev][out, lt, 8:8 + rows, :] = own_sum(lambda i: src[i, lt], out, src.shape[0])

    def send_rows(lev):
        zz, snd, rcv = z[lev], ys[lev], yr[lev]
        m, rows = zz.shape[0] - 2, zz.shape[2] - 16
        snd[0] = W0 * zz[:, :, 6 + rows:7 + rows, :] + W1 * zz[:, :, 7 + rows:8 + rows, :]
        snd[1] = W0 * zz[:, :, 8:9, :]
        waits = []
        for i, d in enumerate((1, -1)):
            for k, (steps, part) in enumerate((
                    ({"gy": d}, pl.ds(0, m)),
                    ({"gz": 1, "gy": d}, pl.ds(m, 1)),
                    ({"gz": -1, "gy": d}, pl.ds(m + 1, 1)))):
                waits.append(send(steps, snd.at[i, part], rcv.at[i, part],
                                  ysend.at[6 * lev + 3 * i + k], yrecv.at[6 * lev + 3 * i + k]))
        return waits

    def send_sections(lev):
        zz = z[lev]
        m, rows = zz.shape[0] - 2, zz.shape[2] - 16
        return [
            send({"gz": d}, zz.at[m + i, :, pl.ds(8, rows), :], zr[lev].at[i],
                 zsend.at[2 * lev + i], zrecv.at[2 * lev + i])
            for i, d in enumerate((1, -1))]

    def take_sections(lev, waits):
        zz = z[lev]
        m, rows = zz.shape[0] - 2, zz.shape[2] - 16
        for i, (d, s) in enumerate(((-1, 0), (1, m - 1))):
            waits[i]()

            @pl.when(has["gz", d])
            def _():
                zz[s, :, 8:8 + rows, :] += zr[lev][i]

    def row_sum(lev, s, lt):
        zz = z[lev]
        half = (zz.shape[2] - 16) // 2

        def load(k):
            return zz[s, lt, pl.ds(6 + k, half, 2), :]
        t[lev][lt, s] = W0 * (load(0) + load(4)) + W1 * (load(1) + load(3)) + W2 * load(2)

    def take_rows(lev, lt):
        tt, rcv = t[lev], yr[lev]
        m, rows = tt.shape[1], tt.shape[2]
        for i, r in enumerate((0, rows - 1)):
            for s in range(m):
                add = rcv[i, s, lt]
                if s == 0:
                    add = add + rcv[i, m, lt]
                if s == m - 1:
                    add = add + rcv[i, m + 1, lt]
                tt[lt, s, r:r + 1, :] += add

    def tile_of(tt, i):
        x = tt[i]
        return x.reshape(x.shape[0] * x.shape[1], LANES)

    def main_tile(lev, j):
        tiles = t[lev].shape[0] - 1
        ids = ((2 * j - 1) % (tiles + 1), 2 * j, 2 * j + 1, 2 * j + 2)
        return dots([tile_of(t[lev], i) for i in ids], wm[...])

    def halo_tile(lev):
        tiles = t[lev].shape[0] - 1
        out = dots([tile_of(t[lev], i) for i in (tiles - 1, tiles, 0)], wh[...])
        lane = lax.broadcasted_iota(jnp.int32, out.shape, 1)
        keep_hi = jnp.where(has["gx", 1], 1, 0)
        keep_lo = jnp.where(has["gx", -1], 1, 0)
        keep = jnp.where(lane < LANES // 2, keep_hi, keep_lo)
        return jnp.where(keep > 0, out, 0.0)

    def put(l, j, x):
        l[:, j] = x.reshape(l.shape[0], l.shape[2], LANES)

    def store(l, out):
        for j in range(l.shape[1] - 1):
            out[:, :, j * LANES:(j + 1) * LANES] = l[:, j]

    m, ny1, nt1 = nz // 2, ny // 2, nt // 2
    ends = (0, m - 1, m, m + 1)
    loads[0].wait()
    loads[1].wait()

    @pl.loop(1, m - 1)
    def _(s):
        sections_first(s, 0, 8)
        sections_first(s, ny - 8, 8)
    for s in ends:
        sections_first(s, 0, 8)
        sections_first(s, ny - 8, 8)
    rows_wait = send_rows(0)
    loads[2].wait()
    for s in (m, m + 1):
        sections_first(s, 8, ny - 16)
    sections_wait = send_sections(0)
    for s in (0, m - 1):
        sections_first(s, 8, ny - 16)

    @pl.loop(1, m - 1)
    def _(s):
        sections_first(s, 8, ny - 16)
        for lt in range(nt):
            row_sum(0, s, lt)
    take_sections(0, sections_wait)
    for s in (0, m - 1):
        for lt in range(nt):
            row_sum(0, s, lt)
    for w in rows_wait:
        w()
    take_rows(0, 0)
    take_rows(0, nt - 1)
    xs_lo[...] = tile_of(t[0], 0).T[0:8, :]
    xs_hi[...] = tile_of(t[0], nt - 1).T[LANES - 16:LANES, :]
    columns_wait = [
        send({"gx": 1}, xs_hi, xr.at[pl.ds(LANES - 16, 16)], xsend.at[0], xrecv.at[0]),
        send({"gx": -1}, xs_lo, xr.at[pl.ds(0, 8)], xsend.at[1], xrecv.at[1])]
    for lt in range(1, nt - 1):
        take_rows(0, lt)
    for j in range(1, nt1 - 1):
        put(l1, j, main_tile(0, j))
    for w in columns_wait:
        w()
    t[0][nt] = xr[...].T.reshape(m, ny1, LANES)
    for j in (0, nt1 - 1):
        put(l1, j, main_tile(0, j))
    put(l1, nt1, halo_tile(0))

    for lev, src, out in ((1, l1, out1), (2, l2, out2)):
        m = src.shape[0] // 2
        for s in (m, m + 1):
            sections_next(lev, src, s)
        sections_wait = send_sections(lev)
        for s in range(m):
            sections_next(lev, src, s)
        rows_wait = send_rows(lev)
        store(src, out)
        for s in range(1, m - 1):
            for lt in range(src.shape[1]):
                row_sum(lev, s, lt)
        take_sections(lev, sections_wait)
        for s in (0, m - 1):
            for lt in range(src.shape[1]):
                row_sum(lev, s, lt)
        for w in rows_wait:
            w()
        for lt in range(src.shape[1]):
            take_rows(lev, lt)
        for j in range((src.shape[1] - 1) // 2):
            if lev == 1:
                put(l2, j, main_tile(lev, j))
            else:
                out3[:, :, j * LANES:(j + 1) * LANES] = main_tile(lev, j).reshape(
                    out3.shape[0], out3.shape[1], LANES)
        if lev == 1:
            put(l2, (src.shape[1] - 1) // 2, halo_tile(lev))

    for steps, copy in sent:
        @pl.when(exists(steps))
        def _():
            copy.wait_send()


def write_out(a1, a2, a3, out1, out2, out3, sem):
    copies = [
        pltpu.make_async_copy(src, dst, sem.at[i])
        for i, (src, dst) in enumerate(((a1, out1), (a2, out2), (a3, out3)))]
    for c in copies:
        c.start()
    for c in copies:
        c.wait()


def on_device(sizes, volume):
    f32 = jnp.float32
    nz, ny, nx = volume.shape
    nt = nx // LANES
    V = pltpu.VMEM
    tiles = [nt, (nt >> 1) + 1, (nt >> 2) + 1]
    z = [V((2 + (nz >> (l + 1)), tiles[l], (ny >> l) + 16, LANES), f32) for l in range(3)]
    zr = [V((2, tiles[l], ny >> l, LANES), f32) for l in range(3)]
    y = [V((2, 2 + (nz >> (l + 1)), tiles[l], 1, LANES), f32) for l in range(3)]
    lv = [V((nz >> l, tiles[l], ny >> l, LANES), f32) for l in (1, 2)]
    t = [V(((nt >> l) + 1, nz >> (l + 1), ny >> (l + 1), LANES), f32) for l in range(3)]
    packed = (nz >> 1) * (ny >> 1)
    dma = pltpu.SemaphoreType.DMA
    hbm = pl.BlockSpec(memory_space=pltpu.HBM)
    vmem = pl.BlockSpec(memory_space=pltpu.VMEM)
    volume = pltpu.with_memory_space_constraint(volume, pltpu.HBM)
    levels = pl.pallas_call(
        functools.partial(kernel, sizes, nz, ny, nt),
        out_shape=tuple(
            V((nz >> l, ny >> l, nx >> l), f32) for l in (1, 2, 3)),
        in_specs=[hbm],
        out_specs=(vmem, vmem, vmem),
        scratch_shapes=[
            V((nz, ny, nx), f32), z, zr, y, y, t, *lv,
            V((8, packed), f32), V((16, packed), f32), V((LANES, packed), f32),
            V((4 * LANES, LANES), jnp.bfloat16), V((3 * LANES, LANES), jnp.bfloat16),
            dma((3,)),
            dma((6,)), dma((6,)), dma((18,)), dma((18,)), dma((2,)), dma((2,)),
        ],
        compiler_params=pltpu.CompilerParams(
            collective_id=0, has_side_effects=True, vmem_limit_bytes=40 << 20),
        name="pyramid",
    )(volume)
    return pl.pallas_call(
        write_out,
        out_shape=tuple(jax.ShapeDtypeStruct(x.shape, f32) for x in levels),
        in_specs=[vmem] * 3,
        out_specs=(hbm, hbm, hbm),
        scratch_shapes=[dma((3,))],
        compiler_params=pltpu.CompilerParams(vmem_limit_bytes=4 << 20),
        name="write_out",
    )(*levels)


def solution(mesh):
    sizes = {a: mesh.shape[a] for a in AXES}
    spec = P(*AXES)
    return jax.shard_map(
        functools.partial(on_device, sizes), mesh=mesh, in_specs=(spec,),
        out_specs=(spec, spec, spec), check_vma=False)
```

```python
import functools

import jax
import jax.numpy as jnp
from jax import lax
from jax.experimental import pallas as pl
from jax.experimental.pallas import tpu as pltpu
from jax.sharding import PartitionSpec as P

LANES = 128
MESH = pl.DeviceIdType.MESH
AXES = ("gz", "gy", "gx")
W0, W1, W2 = 0.0625, 0.25, 0.375


def taps_of(delta):
    far = jnp.abs(delta)
    return jnp.where(
        far == 0, W2, jnp.where(far == 1, W1, jnp.where(far == 2, W0, 0.0))
    ).astype(jnp.bfloat16)


def column_weights():
    row = lax.broadcasted_iota(jnp.int32, (LANES, LANES), 0)
    col = lax.broadcasted_iota(jnp.int32, (LANES, LANES), 1)
    before = taps_of(row - LANES - 2 * col)
    first = taps_of(row - 2 * col)
    second = taps_of(row + LANES - 2 * col)
    after = taps_of(row + 2 * LANES - 2 * col)
    half = LANES // 2
    signed_in = jnp.where(row < half, row, row - LANES)
    signed_out = jnp.where(col < half, col, col - LANES)
    same_side = (row < half) == (col < half)
    halo = taps_of(jnp.where(same_side, signed_in - 2 * signed_out, LANES))
    return before, first, second, after, halo


def split3(x):
    hi = x.astype(jnp.bfloat16)
    rest = x - hi.astype(jnp.float32)
    mid = rest.astype(jnp.bfloat16)
    lo = (rest - mid.astype(jnp.float32)).astype(jnp.bfloat16)
    return hi, mid, lo


def dots(tiles, weights):
    parts = [split3(t) for t in tiles]
    total = None
    for p in (2, 1, 0):
        lhs = jnp.concatenate([q[p] for q in parts], axis=1)
        d = jnp.dot(lhs, weights, preferred_element_type=jnp.float32)
        total = d if total is None else total + d
    return total


def kernel(sizes, dims, vol, out1, out2, out3,
           v, z, t, sh, rz_lo, rz_hi, ys_lo, ys_hi, yr_lo, yr_hi, xs, xr, wm, wh,
           load_sem, zsend, zrecv, ysend, yrecv, xsend, xrecv):
    nz, ny, nt = dims
    idx = {a: lax.axis_index(a) for a in AXES}
    has = {}
    near = {}
    for a in AXES:
        has[a, -1], has[a, 1] = idx[a] > 0, idx[a] < sizes[a] - 1
        near[a, -1] = jnp.maximum(idx[a] - 1, 0)
        near[a, 1] = jnp.minimum(idx[a] + 1, sizes[a] - 1)

    def flag(a, d):
        return jnp.where(has[a, d], 1.0, 0.0).astype(jnp.float32)

    def exists(steps):
        found = None
        for a, d in steps.items():
            found = has[a, d] if found is None else jnp.logical_and(found, has[a, d])
        return found

    def device(steps):
        return {a: near[a, d] for a, d in steps.items()}

    groups = ((0, ny // 2), (ny // 2, ny // 2))
    loads = []
    for g, (r0, rn) in enumerate(groups):
        c = pltpu.make_async_copy(
            vol.at[:, pl.ds(r0, rn), :], v.at[:, pl.ds(r0, rn), :], load_sem.at[g])
        c.start()
        loads.append(c)

    xr[...] = jnp.zeros(xr.shape, jnp.float32)
    for lev in range(3):
        yr_lo[lev][...] = jnp.zeros(yr_lo[lev].shape, jnp.float32)
        yr_hi[lev][...] = jnp.zeros(yr_hi[lev].shape, jnp.float32)

    corners = [{"gz": i, "gy": j} for i in (-1, 1) for j in (-1, 1)]
    peers = [{a: d} for a in AXES for d in (-1, 1)] + corners
    barrier = pltpu.get_barrier_semaphore()
    for p in peers:
        @pl.when(exists(p))
        def _():
            pl.semaphore_signal(barrier, inc=1, device_id=device(p), device_id_type=MESH)

    for lev in range(3):
        pad = z[lev].shape[:2]
        rows = z[lev].shape[2] - 32
        first_pad = 8 + rows if lev == 0 else 16 + rows
        if lev == 0:
            z[lev][:, :, 0:8, :] = jnp.zeros(pad + (8, LANES), jnp.float32)
        z[lev][:, :, first_pad:32 + rows, :] = jnp.zeros(
            pad + (32 + rows - first_pad, LANES), jnp.float32)
    before, first, second, after, halo = column_weights()
    for i, m in enumerate((before, first, second, after)):
        wm[i * LANES:(i + 1) * LANES] = m
    for i, m in enumerate((before, halo, after)):
        wh[i * LANES:(i + 1) * LANES] = m

    sent = []

    def send(steps, src, dst, send_sem, recv_sem):
        copy = pltpu.make_async_remote_copy(
            src_ref=src, dst_ref=dst, send_sem=send_sem, recv_sem=recv_sem,
            device_id=device(steps), device_id_type=MESH)

        @pl.when(exists(steps))
        def _():
            copy.start()
        sent.append((steps, copy))

        def wait():
            @pl.when(exists({a: -d for a, d in steps.items()}))
            def _():
                copy.wait_recv()
        return wait

    tap = {0: W2, 1: W1, 2: W0}
    fz_lo, fz_hi = flag("gz", -1), flag("gz", 1)
    fy_lo, fy_hi = flag("gy", -1), flag("gy", 1)

    def own_sum(load, o, n, ghosts_hi, last):
        if not isinstance(o, int):
            c = 2 * o
            return W0 * (load(c - 2) + load(c + 2)) + W1 * (load(c - 1) + load(c + 1)) \
                + W2 * load(c)
        total = None
        for i in range(2 * o - 2, 2 * o + 3):
            if i < (-1 if ghosts_hi else 0) or i >= n + ghosts_hi:
                continue
            term = tap[abs(i - 2 * o)] * load(i if i >= 0 else last)
            total = term if total is None else total + term
        if o < 0:
            total = total * fz_lo
        elif o >= n // 2:
            total = total * fz_hi
        return total

    def row_sum(lev, s, lt):
        zz = z[lev]
        half = (zz.shape[2] - 32) // 2

        def load(k):
            return zz[s, lt, pl.ds(6 + k, half + 8, 2), :]
        x = W0 * (load(0) + load(4)) + W1 * (load(1) + load(3)) + W2 * load(2)
        lo = (W1 * zz[s, lt, 7:8, :] + W0 * zz[s, lt, 8:9, :]) * fy_lo
        row = lax.broadcasted_iota(jnp.int32, (8, LANES), 0)
        ghost = jnp.where(row < 2, x[half:half + 8] * fy_hi, jnp.where(row == 7, lo, 0.0))
        t[lev][lt, s, 0:half, :] = x[0:half]
        t[lev][lt, s, half:half + 8, :] = ghost

    def tile_of(tt, i):
        x = tt[i]
        return x.reshape(x.shape[0] * x.shape[1], LANES)

    def put(lev, j, x):
        out = sh[lev]
        out[:, j] = x.reshape(out.shape[0], out.shape[2], LANES)

    def columns(lev, tiles):
        tt = t[lev]
        for j in range(tiles // 2):
            ids = [2 * j - 1, 2 * j, 2 * j + 1, 2 * j + 2]
            lo, hi = 0, 4
            if j == 0:
                ids[0] = tiles
                lo = 1 if lev == 0 else 0
            if j == tiles // 2 - 1 and lev == 0:
                hi = 3
            put(lev, j, dots([tile_of(tt, i) for i in ids[lo:hi]], wm[lo * LANES:hi * LANES]))
        if lev == 0:
            w = jnp.concatenate([wh[0:LANES], wh[2 * LANES:3 * LANES]], axis=0)
            out = dots([tile_of(tt, tiles - 1), tile_of(tt, 0)], w)
        else:
            out = dots([tile_of(tt, i) for i in (tiles - 1, tiles, 0)], wh[...])
        lane = lax.broadcasted_iota(jnp.int32, out.shape, 1)
        keep_hi = jnp.where(has["gx", 1], 1, 0)
        keep_lo = jnp.where(has["gx", -1], 1, 0)
        keep = jnp.where(lane < LANES // 2, keep_hi, keep_lo)
        put(lev, tiles // 2, jnp.where(keep > 0, out, 0.0))

    def send_shares(lev):
        s = sh[lev]
        n, rows = nz >> (lev + 1), s.shape[2] - 8
        g = s.shape[0] - n - 1
        ys_hi[lev][...] = s[:, :, rows:rows + g, :]
        ys_lo[lev][...] = s[:, :, rows + 7:rows + 8, :]
        ups, downs, sections = [], [], []
        for i, (d, snd, rcv, waits) in enumerate((
                (1, ys_hi[lev], yr_lo[lev], ups), (-1, ys_lo[lev], yr_hi[lev], downs))):
            for k, (steps, part) in enumerate((
                    ({"gy": d}, pl.ds(0, n)),
                    ({"gz": 1, "gy": d}, pl.ds(n, g)),
                    ({"gz": -1, "gy": d}, pl.ds(n + g, 1)))):
                at = 6 * lev + 3 * i + k
                waits.append(send(steps, snd.at[part], rcv.at[part], ysend.at[at], yrecv.at[at]))
        sections.append(send(
            {"gz": 1}, s.at[pl.ds(n, g), :, pl.ds(0, rows), :], rz_lo[lev],
            zsend.at[2 * lev], zrecv.at[2 * lev]))
        sections.append(send(
            {"gz": -1}, s.at[pl.ds(n + g, 1), :, pl.ds(0, rows), :], rz_hi[lev],
            zsend.at[2 * lev + 1], zrecv.at[2 * lev + 1]))
        return sections, ups + downs

    def take_sections(lev, waits):
        s = sh[lev]
        n, rows = nz >> (lev + 1), s.shape[2] - 8
        g = s.shape[0] - n - 1
        waits[0]()

        @pl.when(has["gz", -1])
        def _():
            s[0:g, :, 0:rows, :] += rz_lo[lev][...]
        waits[1]()

        @pl.when(has["gz", 1])
        def _():
            s[n - 1:n, :, 0:rows, :] += rz_hi[lev][...]

    def take_rows(lev, waits):
        s = sh[lev]
        n, rows = nz >> (lev + 1), s.shape[2] - 8
        g = s.shape[0] - n - 1
        for w in waits:
            w()
        for rcv, r, h in ((yr_lo[lev], 0, g), (yr_hi[lev], rows - 1, 1)):
            for i in range(n):
                add = rcv[i]
                if i < g:
                    add = add + rcv[n + i]
                if i == n - 1:
                    add = add + rcv[n + g]
                s[i, :, r:r + h, :] += add

    m = nz // 2

    def sections_first(o, at, r0, rn):
        for r in range(r0, r0 + rn, 8):
            for lt in range(nt):
                cols = slice(lt * LANES, (lt + 1) * LANES)
                z[0][at, lt, 8 + r:16 + r, :] = own_sum(
                    lambda i: v[i, r:r + 8, cols], o, nz, 0, 0)

    for c, (r0, rn) in zip(loads, groups):
        c.wait()

        @pl.loop(1, m - 1)
        def _(o):
            sections_first(o, o, r0, rn)
        for o, at in ((0, 0), (m - 1, m - 1), (m, m), (-1, m + 1)):
            sections_first(o, at, r0, rn)

    @pl.loop(0, m + 2)
    def _(o):
        for lt in range(nt):
            row_sum(0, o, lt)
    columns(0, nt)
    pl.semaphore_wait(barrier, sum(exists(p).astype(jnp.int32) for p in peers))
    waits = [send_shares(0)]

    for lev in (1, 2):
        src = sh[lev - 1]
        n = nz >> lev
        rows = src.shape[2] - 8
        g = src.shape[0] - n - 1
        tiles = src.shape[1] - 1
        outs = [(o, o) for o in range(n // 2 + 2)] + [(-1, n // 2 + 2)]
        for o, at in outs:
            for lt in range(tiles + 1):
                x = own_sum(lambda i: src[i, lt], o, n, g, n + g)
                z[lev][at, lt, 8:16 + rows, :] = x
                z[lev][at, lt, 0:8, :] = x[rows:rows + 8]
        for o, at in outs:
            for lt in range(tiles + 1):
                row_sum(lev, at, lt)
        columns(lev, tiles)
        waits.append(send_shares(lev))

    for lev in range(3):
        take_sections(lev, waits[lev][0])
    for lev in range(3):
        take_rows(lev, waits[lev][1])
    outs = (out1, out2, out3)
    flat = []
    for lev in range(3):
        n, rows, last = nz >> (lev + 1), sh[lev].shape[2] - 8, sh[lev].shape[1] - 1
        flat.append(sh[lev][0:n, last, 0:rows, :].reshape(n * rows, LANES))
    used = sum(f.shape[0] for f in flat)
    if xr.shape[1] > used:
        flat.append(jnp.zeros((xr.shape[1] - used, LANES), jnp.float32))
    packed = jnp.concatenate(flat, axis=0).T
    xs[0:8, :] = packed[0:8, :]
    xs[8:16, :] = packed[LANES - 8:LANES, :]
    columns_wait = [
        send({"gx": 1}, xs.at[pl.ds(0, 8)], xr.at[pl.ds(0, 8)], xsend.at[0], xrecv.at[0]),
        send({"gx": -1}, xs.at[pl.ds(8, 8)], xr.at[pl.ds(LANES - 8, 8)], xsend.at[1],
             xrecv.at[1])]

    def store(lev, j, x):
        outs[lev][:, :, j * LANES:(j + 1) * LANES] = x

    for lev in range(3):
        n, rows, count = nz >> (lev + 1), sh[lev].shape[2] - 8, sh[lev].shape[1] - 1
        for j in range(1, count - 1):
            store(lev, j, sh[lev][0:n, j, 0:rows, :])
    for w in columns_wait:
        w()
    back = xr[...].T
    start = 0
    for lev in range(3):
        n, rows, count = nz >> (lev + 1), sh[lev].shape[2] - 8, sh[lev].shape[1] - 1
        add = back[start:start + n * rows].reshape(n, rows, LANES)
        start += n * rows
        lane = lax.broadcasted_iota(jnp.int32, add.shape, 2)
        at_lo = jnp.where(lane < 2, add, 0.0)
        at_hi = jnp.where(lane == LANES - 1, add, 0.0)
        x = sh[lev][0:n, 0, 0:rows, :] + at_lo
        if count == 1:
            store(lev, 0, x + at_hi)
        else:
            store(lev, 0, x)
            store(lev, count - 1, sh[lev][0:n, count - 1, 0:rows, :] + at_hi)

    for steps, copy in sent:
        @pl.when(exists(steps))
        def _():
            copy.wait_send()


def write_out(a1, a2, a3, out1, out2, out3, sem):
    copies = [
        pltpu.make_async_copy(src, dst, sem.at[i])
        for i, (src, dst) in enumerate(((a1, out1), (a2, out2), (a3, out3)))]
    for c in copies:
        c.start()
    for c in copies:
        c.wait()


def on_device(sizes, volume):
    f32 = jnp.float32
    nz, ny, nx = volume.shape
    nt = nx // LANES
    V = pltpu.VMEM
    extra = (2, 3, 3)
    ins = (nt, (nt >> 1) + 1, (nt >> 2) + 1)
    n = [nz >> (l + 1) for l in range(3)]
    rows = [ny >> (l + 1) for l in range(3)]
    outs = [(nt >> (l + 1)) + 1 for l in range(3)]
    levels = range(3)
    z = [V((n[l] + extra[l], ins[l], 2 * rows[l] + 32, LANES), f32) for l in levels]
    t = [V((ins[l], n[l] + extra[l], rows[l] + 8, LANES), f32) for l in levels]
    sh = [V((n[l] + extra[l], outs[l], rows[l] + 8, LANES), f32) for l in levels]
    rz_lo = [V((extra[l] - 1, outs[l], rows[l], LANES), f32) for l in levels]
    rz_hi = [V((1, outs[l], rows[l], LANES), f32) for l in levels]
    lows = [V((n[l] + extra[l], outs[l], 1, LANES), f32) for l in levels]
    highs = [V((n[l] + extra[l], outs[l], extra[l] - 1, LANES), f32) for l in levels]
    packed = -(-sum(n[l] * rows[l] for l in levels) // LANES) * LANES
    dma = pltpu.SemaphoreType.DMA
    hbm = pl.BlockSpec(memory_space=pltpu.HBM)
    vmem = pl.BlockSpec(memory_space=pltpu.VMEM)
    volume = pltpu.with_memory_space_constraint(volume, pltpu.HBM)
    results = pl.pallas_call(
        functools.partial(kernel, sizes, (nz, ny, nt)),
        out_shape=tuple(
            V((nz >> l, ny >> l, nx >> l), f32) for l in (1, 2, 3)),
        in_specs=[hbm],
        out_specs=(vmem, vmem, vmem),
        scratch_shapes=[
            V((nz, ny, nx), f32), z, t, sh, rz_lo, rz_hi, lows, highs, highs, lows,
            V((16, packed), f32), V((LANES, packed), f32),
            V((4 * LANES, LANES), jnp.bfloat16), V((3 * LANES, LANES), jnp.bfloat16),
            dma((3,)),
            dma((6,)), dma((6,)), dma((18,)), dma((18,)), dma((2,)), dma((2,)),
        ],
        compiler_params=pltpu.CompilerParams(
            collective_id=0, has_side_effects=True, vmem_limit_bytes=40 << 20),
        name="pyramid",
    )(volume)
    return pl.pallas_call(
        write_out,
        out_shape=tuple(jax.ShapeDtypeStruct(x.shape, f32) for x in results),
        in_specs=[vmem] * 3,
        out_specs=(hbm, hbm, hbm),
        scratch_shapes=[dma((3,))],
        compiler_params=pltpu.CompilerParams(vmem_limit_bytes=4 << 20),
        name="write_out",
    )(*results)


def solution(mesh):
    sizes = {a: mesh.shape[a] for a in AXES}
    spec = P(*AXES)
    return jax.shard_map(
        functools.partial(on_device, sizes), mesh=mesh, in_specs=(spec,),
        out_specs=(spec, spec, spec), check_vma=False)
```

```python
import functools

import jax
import jax.numpy as jnp
from jax import lax
from jax.experimental import pallas as pl
from jax.experimental.pallas import tpu as pltpu
from jax.sharding import PartitionSpec as P

LANES = 128
MESH = pl.DeviceIdType.MESH
AXES = ("gz", "gy", "gx")
W0, W1, W2 = 0.0625, 0.25, 0.375


def taps_of(delta):
    far = jnp.abs(delta)
    return jnp.where(
        far == 0, W2, jnp.where(far == 1, W1, jnp.where(far == 2, W0, 0.0))
    ).astype(jnp.bfloat16)


def column_weights():
    row = lax.broadcasted_iota(jnp.int32, (LANES, LANES), 0)
    col = lax.broadcasted_iota(jnp.int32, (LANES, LANES), 1)
    before = taps_of(row - LANES - 2 * col)
    first = taps_of(row - 2 * col)
    second = taps_of(row + LANES - 2 * col)
    after = taps_of(row + 2 * LANES - 2 * col)
    half = LANES // 2
    signed_in = jnp.where(row < half, row, row - LANES)
    signed_out = jnp.where(col < half, col, col - LANES)
    same_side = (row < half) == (col < half)
    halo = taps_of(jnp.where(same_side, signed_in - 2 * signed_out, LANES))
    return before, first, second, after, halo


def split3(x):
    hi = x.astype(jnp.bfloat16)
    rest = x - hi.astype(jnp.float32)
    mid = rest.astype(jnp.bfloat16)
    lo = (rest - mid.astype(jnp.float32)).astype(jnp.bfloat16)
    return hi, mid, lo


def dots(parts, weights):
    total = None
    for p in (2, 1, 0):
        lhs = jnp.concatenate([q[p] for q in parts], axis=1)
        d = jnp.dot(lhs, weights, preferred_element_type=jnp.float32)
        total = d if total is None else total + d
    return total


def kernel(sizes, dims, vol, out1, out2, out3,
           v, z, t, sh, rz_lo, rz_hi, ys_lo, ys_hi, yr_lo, yr_hi, xs, xr, wm, wh,
           load_sem, zsend, zrecv, ysend, yrecv, xsend, xrecv):
    nz, ny, nt = dims
    idx = {a: lax.axis_index(a) for a in AXES}
    has = {}
    near = {}
    for a in AXES:
        has[a, -1], has[a, 1] = idx[a] > 0, idx[a] < sizes[a] - 1
        near[a, -1] = jnp.maximum(idx[a] - 1, 0)
        near[a, 1] = jnp.minimum(idx[a] + 1, sizes[a] - 1)

    def flag(a, d):
        return jnp.where(has[a, d], 1.0, 0.0).astype(jnp.float32)

    def exists(steps):
        found = None
        for a, d in steps.items():
            found = has[a, d] if found is None else jnp.logical_and(found, has[a, d])
        return found

    def device(steps):
        return {a: near[a, d] for a, d in steps.items()}

    step = 16 if ny % 16 == 0 else 8
    groups = [(r, step) for r in range(0, ny, step)]
    loads = []
    for g, (r0, rn) in enumerate(groups):
        c = pltpu.make_async_copy(
            vol.at[:, pl.ds(r0, rn), :], v.at[:, pl.ds(r0, rn), :], load_sem.at[g])
        c.start()
        loads.append(c)

    xr[...] = jnp.zeros(xr.shape, jnp.float32)
    for lev in range(3):
        yr_lo[lev][...] = jnp.zeros(yr_lo[lev].shape, jnp.float32)
        yr_hi[lev][...] = jnp.zeros(yr_hi[lev].shape, jnp.float32)

    corners = [{"gz": i, "gy": j} for i in (-1, 1) for j in (-1, 1)]
    peers = [{a: d} for a in AXES for d in (-1, 1)] + corners
    barrier = pltpu.get_barrier_semaphore()
    for p in peers:
        @pl.when(exists(p))
        def _():
            pl.semaphore_signal(barrier, inc=1, device_id=device(p), device_id_type=MESH)

    for lev in range(3):
        pad = z[lev].shape[:2]
        rows = z[lev].shape[2] - 32
        first_pad = 8 + rows if lev == 0 else 16 + rows
        if lev == 0:
            z[lev][:, :, 0:8, :] = jnp.zeros(pad + (8, LANES), jnp.float32)
        z[lev][:, :, first_pad:32 + rows, :] = jnp.zeros(
            pad + (32 + rows - first_pad, LANES), jnp.float32)
    before, first, second, after, halo = column_weights()
    for i, m in enumerate((before, first, second, after)):
        wm[i * LANES:(i + 1) * LANES] = m
    for i, m in enumerate((before, halo, after)):
        wh[i * LANES:(i + 1) * LANES] = m

    sent = []

    def send(steps, src, dst, send_sem, recv_sem):
        copy = pltpu.make_async_remote_copy(
            src_ref=src, dst_ref=dst, send_sem=send_sem, recv_sem=recv_sem,
            device_id=device(steps), device_id_type=MESH)

        @pl.when(exists(steps))
        def _():
            copy.start()
        sent.append((steps, copy))

        def wait():
            @pl.when(exists({a: -d for a, d in steps.items()}))
            def _():
                copy.wait_recv()
        return wait

    tap = {0: W2, 1: W1, 2: W0}
    fz_lo, fz_hi = flag("gz", -1), flag("gz", 1)
    fy_lo, fy_hi = flag("gy", -1), flag("gy", 1)

    def own_sum(load, o, n, ghosts_hi, last):
        if not isinstance(o, int):
            c = 2 * o
            return W0 * (load(c - 2) + load(c + 2)) + W1 * (load(c - 1) + load(c + 1)) \
                + W2 * load(c)
        total = None
        for i in range(2 * o - 2, 2 * o + 3):
            if i < (-1 if ghosts_hi else 0) or i >= n + ghosts_hi:
                continue
            term = tap[abs(i - 2 * o)] * load(i if i >= 0 else last)
            total = term if total is None else total + term
        if o < 0:
            total = total * fz_lo
        elif o >= n // 2:
            total = total * fz_hi
        return total

    def row_sum(lev, s, lt):
        zz = z[lev]
        half = (zz.shape[2] - 32) // 2

        def load(k):
            return zz[s, lt, pl.ds(6 + k, half + 8, 2), :]
        x = W0 * (load(0) + load(4)) + W1 * (load(1) + load(3)) + W2 * load(2)
        lo = (W1 * zz[s, lt, 7:8, :] + W0 * zz[s, lt, 8:9, :]) * fy_lo
        row = lax.broadcasted_iota(jnp.int32, (8, LANES), 0)
        ghost = jnp.where(row < 2, x[half:half + 8] * fy_hi, jnp.where(row == 7, lo, 0.0))
        t[lev][lt, s, 0:half, :] = x[0:half]
        t[lev][lt, s, half:half + 8, :] = ghost

    def tile_of(tt, i):
        x = tt[i]
        return x.reshape(x.shape[0] * x.shape[1], LANES)

    def put(lev, j, x):
        out = sh[lev]
        out[:, j] = x.reshape(out.shape[0], out.shape[2], LANES)

    def columns(lev, tiles):
        tt = t[lev]
        parts = [split3(tile_of(tt, i)) for i in range(tt.shape[0])]
        for j in range(tiles // 2):
            ids = [2 * j - 1, 2 * j, 2 * j + 1, 2 * j + 2]
            lo, hi = 0, 4
            if j == 0:
                ids[0] = tiles
                lo = 1 if lev == 0 else 0
            if j == tiles // 2 - 1 and lev == 0:
                hi = 3
            put(lev, j, dots([parts[i] for i in ids[lo:hi]], wm[lo * LANES:hi * LANES]))
        if lev == 0:
            w = jnp.concatenate([wh[0:LANES], wh[2 * LANES:3 * LANES]], axis=0)
            out = dots([parts[tiles - 1], parts[0]], w)
        else:
            out = dots([parts[i] for i in (tiles - 1, tiles, 0)], wh[...])
        lane = lax.broadcasted_iota(jnp.int32, out.shape, 1)
        keep_hi = jnp.where(has["gx", 1], 1, 0)
        keep_lo = jnp.where(has["gx", -1], 1, 0)
        keep = jnp.where(lane < LANES // 2, keep_hi, keep_lo)
        put(lev, tiles // 2, jnp.where(keep > 0, out, 0.0))

    def send_shares(lev):
        s = sh[lev]
        n, rows = nz >> (lev + 1), s.shape[2] - 8
        g = s.shape[0] - n - 1
        ys_hi[lev][...] = s[:, :, rows:rows + g, :]
        ys_lo[lev][...] = s[:, :, rows + 7:rows + 8, :]
        ups, downs, sections = [], [], []
        for i, (d, snd, rcv, waits) in enumerate((
                (1, ys_hi[lev], yr_lo[lev], ups), (-1, ys_lo[lev], yr_hi[lev], downs))):
            for k, (steps, part) in enumerate((
                    ({"gy": d}, pl.ds(0, n)),
                    ({"gz": 1, "gy": d}, pl.ds(n, g)),
                    ({"gz": -1, "gy": d}, pl.ds(n + g, 1)))):
                at = 6 * lev + 3 * i + k
                waits.append(send(steps, snd.at[part], rcv.at[part], ysend.at[at], yrecv.at[at]))
        sections.append(send(
            {"gz": 1}, s.at[pl.ds(n, g), :, pl.ds(0, rows), :], rz_lo[lev],
            zsend.at[2 * lev], zrecv.at[2 * lev]))
        sections.append(send(
            {"gz": -1}, s.at[pl.ds(n + g, 1), :, pl.ds(0, rows), :], rz_hi[lev],
            zsend.at[2 * lev + 1], zrecv.at[2 * lev + 1]))
        return sections, ups + downs

    def take_sections(lev, tiles):
        s = sh[lev]
        n, rows = nz >> (lev + 1), s.shape[2] - 8
        g = s.shape[0] - n - 1

        @pl.when(has["gz", -1])
        def _():
            s[0:g, tiles, 0:rows, :] += rz_lo[lev][:, tiles]

        @pl.when(has["gz", 1])
        def _():
            s[n - 1:n, tiles, 0:rows, :] += rz_hi[lev][:, tiles]

    def take_rows(lev, tiles):
        s = sh[lev]
        n, rows = nz >> (lev + 1), s.shape[2] - 8
        g = s.shape[0] - n - 1
        for rcv, r, h in ((yr_lo[lev], 0, g), (yr_hi[lev], rows - 1, 1)):
            for i in range(n):
                add = rcv[i, tiles]
                if i < g:
                    add = add + rcv[n + i, tiles]
                if i == n - 1:
                    add = add + rcv[n + g, tiles]
                s[i, tiles, r:r + h, :] += add

    m = nz // 2

    def sections_first(o, at, r0, rn):
        for r in range(r0, r0 + rn, 8):
            for lt in range(nt):
                cols = slice(lt * LANES, (lt + 1) * LANES)
                z[0][at, lt, 8 + r:16 + r, :] = own_sum(
                    lambda i: v[i, r:r + 8, cols], o, nz, 0, 0)

    for c, (r0, rn) in zip(loads, groups):
        c.wait()

        @pl.loop(1, m - 1)
        def _(o):
            sections_first(o, o, r0, rn)
        for o, at in ((0, 0), (m - 1, m - 1), (m, m), (-1, m + 1)):
            sections_first(o, at, r0, rn)

    @pl.loop(0, m + 2)
    def _(o):
        for lt in range(nt):
            row_sum(0, o, lt)
    columns(0, nt)
    pl.semaphore_wait(barrier, sum(exists(p).astype(jnp.int32) for p in peers))
    waits = [send_shares(0)]

    for lev in (1, 2):
        src = sh[lev - 1]
        n = nz >> lev
        rows = src.shape[2] - 8
        g = src.shape[0] - n - 1
        tiles = src.shape[1] - 1
        outs = [(o, o) for o in range(n // 2 + 2)] + [(-1, n // 2 + 2)]
        for o, at in outs:
            for lt in range(tiles + 1):
                x = own_sum(lambda i: src[i, lt], o, n, g, n + g)
                z[lev][at, lt, 8:16 + rows, :] = x
                z[lev][at, lt, 0:8, :] = x[rows:rows + 8]
        for o, at in outs:
            for lt in range(tiles + 1):
                row_sum(lev, at, lt)
        columns(lev, tiles)
        waits.append(send_shares(lev))

    for lev in range(3):
        for w in waits[lev][0]:
            w()
        take_sections(lev, pl.ds(sh[lev].shape[1] - 1, 1))
    for lev in range(3):
        for w in waits[lev][1]:
            w()
        take_rows(lev, pl.ds(sh[lev].shape[1] - 1, 1))
    outs = (out1, out2, out3)
    flat = []
    for lev in range(3):
        n, rows, last = nz >> (lev + 1), sh[lev].shape[2] - 8, sh[lev].shape[1] - 1
        flat.append(sh[lev][0:n, last, 0:rows, :].reshape(n * rows, LANES))
    used = sum(f.shape[0] for f in flat)
    if xr.shape[1] > used:
        flat.append(jnp.zeros((xr.shape[1] - used, LANES), jnp.float32))
    packed = jnp.concatenate(flat, axis=0).T
    xs[0:8, :] = packed[0:8, :]
    xs[8:16, :] = packed[LANES - 8:LANES, :]
    columns_wait = [
        send({"gx": 1}, xs.at[pl.ds(0, 8)], xr.at[pl.ds(0, 8)], xsend.at[0], xrecv.at[0]),
        send({"gx": -1}, xs.at[pl.ds(8, 8)], xr.at[pl.ds(LANES - 8, 8)], xsend.at[1],
             xrecv.at[1])]

    for lev in range(3):
        take_sections(lev, pl.ds(0, sh[lev].shape[1] - 1))
        take_rows(lev, pl.ds(0, sh[lev].shape[1] - 1))

    def store(lev, j, x):
        outs[lev][:, :, j * LANES:(j + 1) * LANES] = x

    for lev in range(3):
        n, rows, count = nz >> (lev + 1), sh[lev].shape[2] - 8, sh[lev].shape[1] - 1
        for j in range(1, count - 1):
            store(lev, j, sh[lev][0:n, j, 0:rows, :])
    for w in columns_wait:
        w()
    back = xr[...].T
    start = 0
    for lev in range(3):
        n, rows, count = nz >> (lev + 1), sh[lev].shape[2] - 8, sh[lev].shape[1] - 1
        add = back[start:start + n * rows].reshape(n, rows, LANES)
        start += n * rows
        lane = lax.broadcasted_iota(jnp.int32, add.shape, 2)
        at_lo = jnp.where(lane < 2, add, 0.0)
        at_hi = jnp.where(lane == LANES - 1, add, 0.0)
        x = sh[lev][0:n, 0, 0:rows, :] + at_lo
        if count == 1:
            store(lev, 0, x + at_hi)
        else:
            store(lev, 0, x)
            store(lev, count - 1, sh[lev][0:n, count - 1, 0:rows, :] + at_hi)

    for steps, copy in sent:
        @pl.when(exists(steps))
        def _():
            copy.wait_send()


def write_out(a1, a2, a3, out1, out2, out3, sem):
    copies = [
        pltpu.make_async_copy(src, dst, sem.at[i])
        for i, (src, dst) in enumerate(((a1, out1), (a2, out2), (a3, out3)))]
    for c in copies:
        c.start()
    for c in copies:
        c.wait()


def on_device(sizes, volume):
    f32 = jnp.float32
    nz, ny, nx = volume.shape
    nt = nx // LANES
    V = pltpu.VMEM
    extra = (2, 3, 3)
    ins = (nt, (nt >> 1) + 1, (nt >> 2) + 1)
    n = [nz >> (l + 1) for l in range(3)]
    rows = [ny >> (l + 1) for l in range(3)]
    outs = [(nt >> (l + 1)) + 1 for l in range(3)]
    levels = range(3)
    z = [V((n[l] + extra[l], ins[l], 2 * rows[l] + 32, LANES), f32) for l in levels]
    t = [V((ins[l], n[l] + extra[l], rows[l] + 8, LANES), f32) for l in levels]
    sh = [V((n[l] + extra[l], outs[l], rows[l] + 8, LANES), f32) for l in levels]
    rz_lo = [V((extra[l] - 1, outs[l], rows[l], LANES), f32) for l in levels]
    rz_hi = [V((1, outs[l], rows[l], LANES), f32) for l in levels]
    lows = [V((n[l] + extra[l], outs[l], 1, LANES), f32) for l in levels]
    highs = [V((n[l] + extra[l], outs[l], extra[l] - 1, LANES), f32) for l in levels]
    packed = -(-sum(n[l] * rows[l] for l in levels) // LANES) * LANES
    dma = pltpu.SemaphoreType.DMA
    hbm = pl.BlockSpec(memory_space=pltpu.HBM)
    vmem = pl.BlockSpec(memory_space=pltpu.VMEM)
    volume = pltpu.with_memory_space_constraint(volume, pltpu.HBM)
    results = pl.pallas_call(
        functools.partial(kernel, sizes, (nz, ny, nt)),
        out_shape=tuple(
            V((nz >> l, ny >> l, nx >> l), f32) for l in (1, 2, 3)),
        in_specs=[hbm],
        out_specs=(vmem, vmem, vmem),
        scratch_shapes=[
            V((nz, ny, nx), f32), z, t, sh, rz_lo, rz_hi, lows, highs, highs, lows,
            V((16, packed), f32), V((LANES, packed), f32),
            V((4 * LANES, LANES), jnp.bfloat16), V((3 * LANES, LANES), jnp.bfloat16),
            dma((ny // 8,)),
            dma((6,)), dma((6,)), dma((18,)), dma((18,)), dma((2,)), dma((2,)),
        ],
        compiler_params=pltpu.CompilerParams(
            collective_id=0, has_side_effects=True, vmem_limit_bytes=40 << 20),
        name="pyramid",
    )(volume)
    return pl.pallas_call(
        write_out,
        out_shape=tuple(jax.ShapeDtypeStruct(x.shape, f32) for x in results),
        in_specs=[vmem] * 3,
        out_specs=(hbm, hbm, hbm),
        scratch_shapes=[dma((3,))],
        compiler_params=pltpu.CompilerParams(vmem_limit_bytes=4 << 20),
        name="write_out",
    )(*results)


def solution(mesh):
    sizes = {a: mesh.shape[a] for a in AXES}
    spec = P(*AXES)
    return jax.shard_map(
        functools.partial(on_device, sizes), mesh=mesh, in_specs=(spec,),
        out_specs=(spec, spec, spec), check_vma=False)
```
